256 devices in a mesh: seq: 32 (over z, x_lo, core), fsdp: 8 (over x_hi, y).
Axes of the slice: x: 4 (x_hi: 2, x_lo: 2; x = x_hi * 2 + x_lo), y: 4, z: 8, core: 2. Of those that a mesh axis runs over, the one named last changes fastest.
Arguments:
- hidden_next: bfloat16 [8192, 8192], P('seq'), may hold values from -6 to 6
- values_next: bfloat16 [8192, 8192], P('seq', 'fsdp'), may hold values from -6 to 6
- seg_next: int32 [4], replicated, may hold values from 1 to 4096, 8192 in all
- proj_bc: bfloat16 [8192, 1024], P(('seq', 'fsdp')), may hold values from -0.09375 to 0.09375
- proj_dt: bfloat16 [8192, 128], P(('seq', 'fsdp')), may hold values from -0.0625 to 0.0625
- dt_bias: float32 [128], replicated, may hold values from -4 to -2.5
- decay_rate: float32 [128], replicated, may hold values from 0 to 1, as said below
- skip_gain: float32 [128], replicated, may hold values from 0.5 to 1.5
- bc_prev: bfloat16 [8192, 1024], P('seq'), may hold values from -4 to 4
- dt_prev: float32 [8192, 128], P('seq', 'fsdp'), may hold values from 0.01 to 0.3
- seg_prev: int32 [4], replicated, may hold values from 1 to 4096, 8192 in all
- grad_prev: bfloat16 [8192, 8192], P('seq', 'fsdp'), may hold values from -6 to 6
Outputs:
- out_next: bfloat16 [8192, 8192], P('seq', 'fsdp')
- grad_values: bfloat16 [8192, 8192], P('seq', 'fsdp')
The draws below stay inside these ranges and needn't reach their ends.
Inputs may be any that keep to these rules, and one draw needn't show every extreme that they name: `seg_next`: lengths of the rollout's 4 segments in order, summing to 8192. `seg_prev`: lengths of the rollout's 4 segments in order, summing to 8192. `decay_rate`: positive.
All inputs are finite; a program needn't handle non-finite values.
Results may differ from the reference program's by a relative error of at most 0.0064.
Values may be sent and summed in bfloat16 or wider, within the bound.
No kernel may reach another device: no remote copies, remote signals or barrier semaphores. Data moves between devices by JAX's collectives and lax.ppermute only.
A program may use at most 128 MiB of HBM per device.

```python
import math
import jax
import jax.numpy as jnp
import numpy as np
from jax import lax

D = 8192
HW = 128
P_SIZE = 64
GW = 4
N = 128
SPAN = 128
NSEG = 4
SEQ_LEN = 8192
BCW = 1024


def draw_decay_rate(key, part):
    streams = jax.random.split(jax.random.fold_in(key, 11), 3)
    lasting = jax.random.uniform(streams[0], (HW,)) < 0.5
    slow_rate = jnp.exp(jax.random.uniform(streams[1], (HW,), minval=jnp.log(5.0), maxval=jnp.log(20.0))) / SEQ_LEN
    fast_rate = jnp.exp(jax.random.uniform(streams[2], (HW,), minval=jnp.log(0.25), maxval=jnp.log(0.8)))
    return jnp.where(lasting, slow_rate, fast_rate).astype(jnp.float32)


def spiked(values, stream_key, source, target, blocks, factor):
    owner, partner = [(jnp.arange(values.shape[position]) // (values.shape[position] // blocks)).reshape([-1 if axis == position else 1 for axis in range(values.ndim)]) for position in (source, target)]
    chosen = jax.random.permutation(stream_key, blocks)[partner]
    strong = (owner == chosen) | (owner == (partner + blocks // 2) % blocks)
    return jnp.where(strong, factor * values, values)


def block_scale(rng, shape, cuts, least, largest):
    def one(axis_at, shards_of):
        heights = jax.random.uniform(jax.random.fold_in(jax.random.fold_in(rng, 6), axis_at), (shards_of,), jnp.float32, least / len(cuts), largest / len(cuts))
        return jnp.repeat(jnp.exp(heights), shape[axis_at] // shards_of).reshape((-1,) + (1,) * (len(shape) - axis_at - 1))

    factor_of = one(*cuts[0])
    for cut in cuts[1:]:
        factor_of = factor_of * one(*cut)
    return factor_of


def split_up(amount, total, reach, lean):
    loads = [(1 << 20) // math.isqrt(rank ** lean) + 1 for rank in range(2, amount + 1)]
    rest, counts = total - reach - (amount - 1), [1] * (amount - 1)
    while rest > 0:
        free = [i for i in range(amount - 1) if counts[i] < reach]
        pool, left = sum([loads[i] for i in free]), rest
        for i in free:
            extra = min(reach - counts[i], max(1, left * loads[i] // pool), rest)
            counts[i] = counts[i] + extra
            rest = rest - extra
    return np.array([reach] + counts)


def uneven(stream_key, count, total, limit, slope):
    if count == 2:
        one = jax.random.randint(stream_key, (), max(1, total - limit), min(limit, total - 1) + 1)
        return jnp.stack([one, total - one])
    sizes = jnp.asarray(split_up(count, total, limit, slope), jnp.int32)
    pairs = (count - 1) // 2
    donor, sink = sizes[1:1 + 2 * pairs:2], sizes[2:2 + 2 * pairs:2]
    slack = jnp.minimum(donor - 1, limit - sink)
    shifted = jax.random.randint(jax.random.fold_in(stream_key, 1), (pairs,), 0, 1 << 20) % (slack + 1)
    sizes = sizes.at[1:1 + 2 * pairs:2].set(donor - shifted).at[2:2 + 2 * pairs:2].set(sink + shifted)
    return sizes[jax.random.permutation(jax.random.fold_in(stream_key, 2), count)]


def noise(own_key, shape, scale, most, pieces=(), kind=jnp.bfloat16):
    factor_of = block_scale(own_key, shape, pieces, -0.22, 0.18) if pieces else 1.0
    drawn = jax.random.normal(own_key, shape, jnp.float32) * scale * factor_of
    return jnp.minimum(jnp.maximum(drawn, -most), most).astype(kind)


def bell_draw_with(stream_key, extent, width, most, cuts, heavy, held_as=jnp.bfloat16):
    entries = width * jax.random.normal(stream_key, extent, jnp.float32)
    if cuts:
        entries = entries * block_scale(stream_key, extent, cuts, -0.22, 0.18)
    return jnp.clip(spiked(entries, jax.random.fold_in(stream_key, 3), *heavy), -most, most).astype(held_as)


def setup_inputs(seed: int = 0) -> dict:
    splits = jax.random.split(jax.random.key(seed), 13)
    hidden_next = noise(splits[0], (SEQ_LEN, D), 1.0, 6.0, ((0, 32),))
    values_next = noise(splits[1], (SEQ_LEN, HW * P_SIZE), 1.0, 6.0, ((0, 32), (1, 8)))
    seg_next = uneven(splits[2], NSEG, SEQ_LEN, SEQ_LEN // 2, 2).astype(jnp.int32)
    proj_bc = bell_draw_with(splits[3], (D, BCW), (D * 8) ** -0.5, 0.09375, ((0, 256),), (0, 1, 256, 6.0))
    proj_dt = noise(splits[4], (D, HW), D ** -0.5, 0.0625, ((0, 256),))
    dt_bias = jnp.clip(jax.random.uniform(splits[5], (HW,), jnp.float32, -4.0, -2.5), -4.0, -2.5)
    decay_rate = draw_decay_rate(jax.random.fold_in(splits[12], 71), 0)
    skip_gain = jnp.clip(jax.random.uniform(splits[7], (HW,), jnp.float32, 0.5, 1.5), 0.5, 1.5)
    bc_prev = noise(splits[8], (SEQ_LEN, BCW), 0.3, 4.0, ((0, 32),))
    dt_prev = jnp.clip(jnp.exp(math.log(0.3) - 3.4011974 * jax.random.uniform(splits[9], (SEQ_LEN, HW), jnp.float32) ** block_scale(splits[9], (SEQ_LEN, HW), ((0, 32), (1, 8)), -0.2, 0.2)), 0.01, 0.3)
    seg_prev = uneven(splits[10], NSEG, SEQ_LEN, SEQ_LEN // 2, 2).astype(jnp.int32)
    grad_prev = noise(splits[11], (SEQ_LEN, HW * P_SIZE), 1.0, 6.0, ((0, 32), (1, 8)))
    return dict(hidden_next=hidden_next, values_next=values_next, seg_next=seg_next, proj_bc=proj_bc, proj_dt=proj_dt, dt_bias=dt_bias, decay_rate=decay_rate, skip_gain=skip_gain, bc_prev=bc_prev, dt_prev=dt_prev, seg_prev=seg_prev, grad_prev=grad_prev)


def segment_table(lengths, tokens_total):
    bounds = jnp.cumsum(lengths)[:-1].astype(jnp.int32)
    places = jnp.arange(tokens_total + 1, dtype=jnp.int32) - 1
    return jnp.sum((bounds[None, :] <= places[:, None]).astype(jnp.int32), axis=1)


def block_parts(bc_block, dt_block, seg_ext, decay_rate):
    span_len = bc_block.shape[0]
    half_cols = bc_block.shape[1] // 2
    b_vectors = bc_block[:, :half_cols].reshape(span_len, GW, N)
    c_vectors = bc_block[:, half_cols:].reshape(span_len, GW, N)
    before = seg_ext[0]
    segment = seg_ext[1:]
    cumulative = jnp.cumsum(-dt_block * decay_rate[None, :], axis=0)
    final_cum = cumulative[-1]
    places = jnp.arange(span_len)
    linked = (segment[:, None] == segment[None, :]) & (places[:, None] >= places[None, :])
    scores = jnp.einsum("tgn,sgn->gts", c_vectors.astype(jnp.float32), b_vectors.astype(jnp.float32),
                        precision=lax.Precision.HIGHEST)
    by_head = cumulative.T
    spread = by_head[:, :, None] - by_head[:, None, :]
    decays = jnp.exp(jnp.where(linked[None], spread, -jnp.inf))
    weighted = (decays * dt_block.T[:, None, :]).reshape(GW, HW // GW, span_len, span_len)
    mixing = (weighted * scores[:, None]).reshape(HW, span_len, span_len).astype(jnp.bfloat16)
    keep_final = (segment == segment[-1]).astype(jnp.float32)
    linked_in = (segment == before).astype(jnp.float32)
    send_factor = keep_final[:, None] * jnp.exp(final_cum[None, :] - cumulative) * dt_block
    read_factor = linked_in[:, None] * jnp.exp(cumulative)
    carry_decay = (segment[-1] == before).astype(jnp.float32) * jnp.exp(final_cum)
    return b_vectors, c_vectors, mixing, send_factor, read_factor, carry_decay


def outer_sum(values, vectors):
    span_len, heads_all, head_dim = values.shape
    grouped = values.reshape(span_len, GW, heads_all // GW, head_dim).astype(jnp.float32)
    result = jnp.einsum("sgqp,sgn->gqpn", grouped, vectors.astype(jnp.float32), precision=lax.Precision.HIGHEST)
    return result.reshape(heads_all, head_dim, vectors.shape[2])


def read_state(state_now, vectors, factor):
    heads_all, head_dim, state_dim = state_now.shape
    grouped = state_now.reshape(GW, heads_all // GW, head_dim, state_dim)
    result = jnp.einsum("gqpn,tgn->tgqp", grouped, vectors.astype(jnp.float32), precision=lax.Precision.HIGHEST)
    return result.reshape(vectors.shape[0], heads_all, head_dim) * factor[:, :, None]


def forward_rollout(hidden, inputs, lengths, proj_bc, proj_dt, dt_bias, decay_rate, skip_gain):
    dt_all = jax.nn.softplus(jnp.dot(hidden, proj_dt, preferred_element_type=jnp.float32) + dt_bias[None, :])
    bc_all = jnp.dot(hidden, proj_bc, preferred_element_type=jnp.float32).astype(jnp.bfloat16)
    seg_all = segment_table(lengths, SEQ_LEN)

    def advance(state_now, block_id):
        offset = (block_id * SPAN).astype(jnp.int32)
        bc_block = lax.dynamic_slice_in_dim(bc_all, offset, SPAN, 0)
        dt_block = lax.dynamic_slice_in_dim(dt_all, offset, SPAN, 0)
        seg_ext = lax.dynamic_slice_in_dim(seg_all, offset, SPAN + 1, 0)
        values = lax.dynamic_slice_in_dim(inputs, offset, SPAN, 0).reshape(SPAN, HW, P_SIZE)
        b_vectors, c_vectors, mixing, send_factor, read_factor, carry_decay = block_parts(
            bc_block, dt_block, seg_ext, decay_rate)
        inside = jnp.einsum("hts,shp->thp", mixing.astype(jnp.float32), values.astype(jnp.float32),
                            precision=lax.Precision.HIGHEST)
        output = inside + read_state(state_now, c_vectors, read_factor) + skip_gain[None, :, None] * values.astype(jnp.float32)
        scaled = (values.astype(jnp.float32) * send_factor[:, :, None]).astype(jnp.bfloat16)
        state_next = carry_decay[:, None, None] * state_now + outer_sum(scaled, b_vectors)
        return state_next, output.astype(jnp.bfloat16).reshape(SPAN, HW * P_SIZE)

    blocks_all = jnp.arange(SEQ_LEN // SPAN, dtype=jnp.int32)
    _, outputs = lax.scan(advance, jnp.zeros((HW, P_SIZE, N), jnp.float32), blocks_all)
    return outputs.reshape(SEQ_LEN, HW * P_SIZE)


def backward_rollout(bc_all, dt_all, lengths, grads_all, decay_rate, skip_gain):
    seg_all = segment_table(lengths, SEQ_LEN)

    def retreat(state_now, block_id):
        offset = (block_id * SPAN).astype(jnp.int32)
        bc_block = lax.dynamic_slice_in_dim(bc_all, offset, SPAN, 0)
        dt_block = lax.dynamic_slice_in_dim(dt_all, offset, SPAN, 0)
        seg_ext = lax.dynamic_slice_in_dim(seg_all, offset, SPAN + 1, 0)
        grad_block = lax.dynamic_slice_in_dim(grads_all, offset, SPAN, 0).reshape(SPAN, HW, P_SIZE)
        b_vectors, c_vectors, mixing, send_factor, read_factor, carry_decay = block_parts(
            bc_block, dt_block, seg_ext, decay_rate)
        inside = jnp.einsum("hts,thp->shp", mixing.astype(jnp.float32), grad_block.astype(jnp.float32),
                            precision=lax.Precision.HIGHEST)
        output = inside + read_state(state_now, b_vectors, send_factor) + skip_gain[None, :, None] * grad_block.astype(jnp.float32)
        scaled = (grad_block.astype(jnp.float32) * read_factor[:, :, None]).astype(jnp.bfloat16)
        state_next = carry_decay[:, None, None] * state_now + outer_sum(scaled, c_vectors)
        return state_next, output.astype(jnp.bfloat16).reshape(SPAN, HW * P_SIZE)

    blocks_all = jnp.arange(SEQ_LEN // SPAN, dtype=jnp.int32)
    _, outputs = lax.scan(retreat, jnp.zeros((HW, P_SIZE, N), jnp.float32), blocks_all, reverse=True)
    return outputs.reshape(SEQ_LEN, HW * P_SIZE)


def reference(hidden_next, values_next, seg_next, proj_bc, proj_dt, dt_bias, decay_rate, skip_gain,
              bc_prev, dt_prev, seg_prev, grad_prev):
    out_next = forward_rollout(hidden_next, values_next, seg_next, proj_bc, proj_dt, dt_bias, decay_rate, skip_gain)
    grad_values = backward_rollout(bc_prev, dt_prev, seg_prev, grad_prev, decay_rate, skip_gain)
    return out_next, grad_values
```

```python
import functools
import jax
import jax.numpy as jnp
from jax import lax
from jax.experimental import pallas as pl
from jax.experimental.pallas import tpu as pltpu
from jax.sharding import Mesh
from jax.sharding import PartitionSpec as P

SEQ = ("z", "xl", "c")
FSDP = ("xh", "y")
BF = jnp.bfloat16
F32 = jnp.float32
T = 256
HEADS = 16
PAIRS = HEADS // 2
NEG = -1e30
VM = pl.BlockSpec(memory_space=pltpu.VMEM)
SM = pl.BlockSpec(memory_space=pltpu.SMEM)


def call(kernel, outs, name, n_smem, args, flops=10_000_000, nbytes=1_000_000):
    return pl.pallas_call(
        kernel,
        out_shape=outs,
        in_specs=[SM] * n_smem + [VM] * (len(args) - n_smem),
        out_specs=jax.tree.map(lambda _: VM, outs),
        name=name,
        cost_estimate=pl.CostEstimate(flops=flops, bytes_accessed=nbytes, transcendentals=0),
    )(*args)


def sds(shape, dtype):
    return jax.ShapeDtypeStruct(shape, dtype)


def lanes(shape):
    return lax.broadcasted_iota(jnp.int32, shape, len(shape) - 1)


def rows(shape):
    return lax.broadcasted_iota(jnp.int32, shape, len(shape) - 2)


def k_columns(sc, bc_ref, dt_ref, out_ref):
    me = sc[7]
    lane = lanes((32, 128))
    low = lane < 64
    for j in range(4):
        b = bc_ref[:, 128 * j : 128 * j + 128].astype(F32)
        c = bc_ref[:, 512 + 128 * j : 640 + 128 * j].astype(F32)
        out_ref[2 * j, 0:32] = jnp.where(low, b, pltpu.roll(c, 64, 1)).astype(BF)
        out_ref[2 * j + 1, 0:32] = jnp.where(low, pltpu.roll(b, 64, 1), c).astype(BF)
    d = dt_ref[...].astype(F32)
    mine = lane // 16 == me
    for k in range(8):
        out_ref[k, 32:64] = jnp.where(mine, pltpu.roll(d, (16 * (me - k)) & 127, 1), 0.0).astype(BF)


def k_rows(rec_ref, out_ref):
    total = jnp.zeros((32, 128), F32)
    for k in range(8):
        out_ref[32 * k : 32 * k + 32] = rec_ref[k, 0:32]
        total = total + rec_ref[k, 32:64].astype(F32)
    out_ref[256:288] = total.astype(BF)


def k_quad(sc, own, other_x, other_c, other_xc, out_ref):
    c, x = sc[4], sc[5]
    out_ref[2 * x + c] = own[...]
    out_ref[2 * (1 - x) + c] = other_x[...]
    out_ref[2 * x + 1 - c] = other_c[...]
    out_ref[2 * (1 - x) + 1 - c] = other_xc[...]


def k_project(sc, hid, q0, r1, g1, r2, g2, r3, g3, h_own, h_other, y_ref, dt_ref):
    c, z = sc[4], sc[6]
    sign = 1 - 2 * c
    spread = (lanes((T, 128)) // 16) == (rows((T, 128)) // 32)

    def block(part):
        packed = part[256:288]
        tall = jnp.concatenate([packed] * 8, axis=0)
        return jnp.concatenate([part[0:256], jnp.where(spread, tall, jnp.zeros_like(tall))], axis=1)

    def times(off, parts):
        width = 256 * len(parts)
        left = hid[:, pl.ds(pl.multiple_of(off, 256), width)]
        right = jnp.concatenate([block(p) for p in parts], axis=0)
        return jnp.dot(left, right, preferred_element_type=F32)

    acc = times(1024 * z, [q0[b] for b in range(4)])
    for r, (up, down) in enumerate(((r1, g1), (r2, g2), (r3, g3)), 1):
        acc = acc + times(1024 * ((z - sign * r) & 7), [up[b] for b in range(4)])
        acc = acc + times(1024 * ((z + sign * r) & 7), [down[b] for b in range(4)])
    far = 1024 * ((z + 4) & 7)
    acc = acc + times(far + 512 * c, [h_own[b] for b in range(2)])
    acc = acc + times(far + 512 * (1 - c), [h_other[b] for b in range(2)])
    y_ref[...] = acc[:, 0:128].astype(BF)
    d = acc[:, 128:256]
    for shift in (16, 32, 64):
        d = d + pltpu.roll(d, shift, 1)
    dt_ref[...] = d


def gather_weights(sc, proj_bc, proj_dt):
    send = call(k_columns, sds((8, 64, 128), BF), "columns", 1, (sc, proj_bc, proj_dt))
    got = lax.all_to_all(send, FSDP, 0, 0, tiled=False)
    own = call(k_rows, sds((288, 128), BF), "rows", 0, (got,))
    swap = [(0, 1), (1, 0)]
    other_x = lax.ppermute(own, "xl", swap)
    other_c = lax.ppermute(own, "c", swap)
    other_xc = lax.ppermute(other_x, "c", swap)
    quad = call(k_quad, sds((4, 288, 128), BF), "quad", 1, (sc, own, other_x, other_c, other_xc))
    ring = [(2 * z, 2 * ((z + 1) % 8)) for z in range(8)] + [(2 * z + 1, 2 * ((z - 1) % 8) + 1) for z in range(8)]
    got, swapped, now = [], [], quad
    for _ in range(3):
        now = lax.ppermute(now, ("z", "c"), ring)
        got.append(now)
        swapped.append(lax.ppermute(now, "c", swap))
    half = lax.dynamic_slice_in_dim(now, 2 * lax.axis_index("c"), 2, 0)
    far = lax.ppermute(half, ("z", "c"), ring)
    far_other = lax.ppermute(far, "c", swap)
    return quad, got[0], swapped[0], got[1], swapped[1], got[2], swapped[2], far, far_other


def segment_of(sc, place):
    return (
        (place >= sc[0]).astype(jnp.int32) + (place >= sc[1]).astype(jnp.int32) + (place >= sc[2]).astype(jnp.int32)
    )


def scalar_segment(sc, place):
    one, none = jnp.int32(1), jnp.int32(0)
    return sum((jnp.where(place >= sc[k], one, none) for k in range(3)), none)


def expand(factor, j, low):
    a = jnp.broadcast_to(factor[:, 2 * j : 2 * j + 1], (T, 128))
    b = jnp.broadcast_to(factor[:, 2 * j + 1 : 2 * j + 2], (T, 128))
    return jnp.where(low, a, b)


def local_part(reverse, sc, dt, decay, b, c, val_ref, outs, scratch):
    keep_ref, send_ref, cum_ref, cumt_ref, dtt_ref, late_ref = outs
    offset, core = sc[3], sc[4]
    before, last = scalar_segment(sc, offset - 1), scalar_segment(sc, offset + T - 1)
    dt_t = jnp.transpose(dt)[0:HEADS]
    x = -jnp.transpose(dt * decay)[0:HEADS]
    lane = lanes((HEADS, T))
    for shift in (1, 2, 4, 8, 16, 32, 64, 128):
        x = x + jnp.where(lane >= shift, pltpu.roll(x, shift, 1), 0.0)
    cum_t = x
    cum = jnp.transpose(jnp.concatenate([cum_t] * 8, axis=0))
    final = cum[T - 1 : T]
    place = offset + rows((T, 128))
    seg = segment_of(sc, place)
    send = jnp.where(seg == last, jnp.exp(final - cum) * dt, 0.0)
    read = jnp.where(seg == before, jnp.exp(cum), 0.0)
    early, late = (read, send) if reverse else (send, read)
    cum_ref[...] = cum
    cumt_ref[...] = cum_t
    dtt_ref[...] = dt_t
    late_ref[...] = late
    low = lanes((T, 128)) < 64
    side = c if reverse else b
    for j in range(PAIRS):
        v = val_ref[:, 128 * j : 128 * j + 128].astype(F32)
        scaled = (v * expand(early, j, low)).astype(BF)
        out = lax.dot_general(scaled, side, (((0,), (0,)), ((), ())), preferred_element_type=F32)
        scratch[j // 4, 128 * (j % 4) : 128 * (j % 4) + 128] = out.astype(BF)
    a = jnp.broadcast_to(jnp.exp(cum_t[:, T - 1 : T]), (HEADS, 128))
    a = jnp.where(last == before, a, 0.0)
    high = a.astype(BF).astype(F32)
    rest = a - high
    for half in range(2):
        pick = slice(8 * half, 8 * half + 8)
        scratch[half, 512:528] = jnp.concatenate([high[pick], rest[pick]], axis=0).astype(BF)
    keep_ref[...] = scratch[core]
    send_ref[...] = scratch[1 - core]


def k_local_prev(sc, dt_ref, par, b_ref, c_ref, val_ref, *refs):
    local_part(True, sc, dt_ref[...], par[0:1], b_ref[...], c_ref[...], val_ref, refs[:6], refs[6])


def softplus(v):
    return jnp.maximum(v, 0.0) + jnp.log1p(jnp.exp(-jnp.abs(v)))


def k_local_next(sc, dt_ref, par, mine_ref, pair_ref, val_ref, *refs):
    outs, b_out, c_out, scratch = refs[:6], refs[6], refs[7], refs[8]
    odd = (sc[7] & 1) == 1
    mine, pair = mine_ref[...].astype(F32), pair_ref[...].astype(F32)
    lo, hi = jnp.where(odd, pair, mine), jnp.where(odd, mine, pair)
    low = lanes((T, 128)) < 64
    b = jnp.where(low, lo, pltpu.roll(hi, 64, 1)).astype(BF)
    c = jnp.where(low, pltpu.roll(lo, 64, 1), hi).astype(BF)
    b_out[...] = b
    c_out[...] = c
    dt = softplus(dt_ref[...] + par[1:2])
    local_part(False, sc, dt, par[0:1], b, c, val_ref, outs, scratch)


LOCAL_OUTS = (
    sds((528, 128), BF),
    sds((528, 128), BF),
    sds((T, 128), F32),
    sds((HEADS, T), F32),
    sds((HEADS, T), F32),
    sds((T, 128), F32),
)


def call_scratch(kernel, outs, name, n_smem, args, scratch, flops):
    return pl.pallas_call(
        kernel,
        out_shape=outs,
        in_specs=[SM] * n_smem + [VM] * (len(args) - n_smem),
        out_specs=jax.tree.map(lambda _: VM, outs),
        scratch_shapes=scratch,
        name=name,
        cost_estimate=pl.CostEstimate(flops=flops, bytes_accessed=2_000_000, transcendentals=0),
    )(*args)


def k_inside(reverse, sc, skip, cum_ref, cumt_ref, dtt_ref, b_ref, c_ref, val_ref, out_ref, bias_ref, score_ref):
    offset, first_head = sc[3], HEADS * sc[7]
    shape = (T, T)
    seg_r = segment_of(sc, offset + rows(shape))
    seg_l = segment_of(sc, offset + lanes(shape))
    causal = rows(shape) <= lanes(shape) if reverse else rows(shape) >= lanes(shape)
    bias_ref[...] = jnp.where((seg_r == seg_l) & causal, 0.0, NEG)
    one, two = (b_ref, c_ref) if reverse else (c_ref, b_ref)
    score_ref[...] = lax.dot_general(one[...], two[...], (((1,), (1,)), ((), ())), preferred_element_type=F32)
    low = lanes((T, 128)) < 64
    cum = cum_ref[...]
    for j in range(PAIRS):
        v = val_ref[:, 128 * j : 128 * j + 128]
        parts = []
        for h in (2 * j, 2 * j + 1):
            col = jnp.broadcast_to(cum[:, h : h + 1], shape)
            row = cumt_ref[h : h + 1]
            if reverse:
                spread = row - col
            else:
                spread = col - row
            decays = jnp.exp(spread + bias_ref[...])
            if reverse:
                mix = (decays * score_ref[...])
            else:
                mix = decays * dtt_ref[h : h + 1] * score_ref[...]
            parts.append(jnp.dot(mix.astype(BF), v, preferred_element_type=F32))
        inside = jnp.where(low, parts[0], parts[1])
        gain = jnp.where(low, skip[first_head + 2 * j], skip[first_head + 2 * j + 1])
        if reverse:
            dt = jnp.transpose(jnp.concatenate([dtt_ref[...]] * 8, axis=0)) if j == 0 else dt
            inside = inside * expand(dt, j, low)
        out_ref[:, 128 * j : 128 * j + 128] = inside + gain * v.astype(F32)


def k_final(sc, base_ref, late_ref, side_ref, keep_ref, got_ref, out_ref, scratch):
    core = sc[4]
    scratch[core] = keep_ref[...]
    scratch[1 - core] = got_ref[...]
    low = lanes((T, 128)) < 64
    late = late_ref[...]
    for j in range(PAIRS):
        st = scratch[j // 4, 128 * (j % 4) : 128 * (j % 4) + 128]
        seen = lax.dot_general(side_ref[...], st, (((1,), (1,)), ((), ())), preferred_element_type=F32)
        at = slice(128 * j, 128 * j + 128)
        out_ref[:, at] = (base_ref[:, at] + expand(late, j, low) * seen).astype(BF)


def decays_of(tail):
    t = tail.astype(F32)
    return t[0:8] + t[8:16]


def tail_of(a):
    high = a.astype(BF).astype(F32)
    return jnp.concatenate([high, a - high], axis=0).astype(BF)


def per_row(a, heads):
    return jnp.concatenate([jnp.broadcast_to(a[h : h + 1], (64, 128)) for h in range(heads)], axis=0)


def quarter_rows(a, which):
    return per_row(jnp.where(which == 0, a[0:4], a[4:8]), 4)


def first_of(reverse, bit):
    return (bit == 1) if reverse else (bit == 0)


def k_core(reverse, sc, own, got, keep_ref, send_ref, scratch):
    core, x = sc[4], sc[5]
    mine_first = first_of(reverse, core)
    so, sg = own[0:512].astype(F32), got[0:512].astype(F32)
    ao, ag = decays_of(own[512:528]), decays_of(got[512:528])
    first, second = jnp.where(mine_first, so, sg), jnp.where(mine_first, sg, so)
    a_second = jnp.where(mine_first, ag, ao)
    joined = (second + per_row(a_second, 8) * first).astype(BF)
    tail = tail_of(ao * ag)
    for q in range(2):
        scratch[q, 0:256] = joined[256 * q : 256 * q + 256]
        scratch[q, 256:272] = tail
    keep_ref[...] = scratch[x]
    send_ref[...] = scratch[1 - x]


def k_chip(reverse, sc, own, got, out_ref):
    x = sc[5]
    mine_first = first_of(reverse, x)
    so, sg = own[0:256].astype(F32), got[0:256].astype(F32)
    ao, ag = decays_of(own[256:272]), decays_of(got[256:272])
    first, second = jnp.where(mine_first, so, sg), jnp.where(mine_first, sg, so)
    a_second = jnp.where(mine_first, ag, ao)
    out_ref[0:256] = (second + quarter_rows(a_second, x) * first).astype(BF)
    out_ref[256:272] = tail_of(ao * ag)


def k_two(sc, near, far, out_ref):
    x = sc[5]
    a = decays_of(near[256:272])
    out_ref[...] = (near[0:256].astype(F32) + quarter_rows(a, x) * far[0:256].astype(F32)).astype(BF)


def k_four(reverse, sc, near, far, pair, older, own, got, keep_ref, send_ref):
    x = sc[5]
    a = decays_of(near[256:272]) * decays_of(far[256:272])
    before = pair[...].astype(F32) + quarter_rows(a, x) * older[...].astype(F32)
    mine_first = first_of(reverse, x)
    first = jnp.where(mine_first, own[0:256].astype(F32), got[0:256].astype(F32))
    a_first = jnp.where(mine_first, decays_of(own[256:272]), decays_of(got[256:272]))
    after = first + quarter_rows(a_first, x) * before
    keep_ref[...] = jnp.where(mine_first, before, after).astype(BF)
    send_ref[...] = jnp.where(mine_first, after, before).astype(BF)


def k_slab(reverse, sc, mine, other, own, got, keep_ref, send_ref, scratch):
    core, x = sc[4], sc[5]
    scratch[x] = mine[...]
    scratch[1 - x] = other[...]
    before = jnp.concatenate([scratch[0], scratch[1]], axis=0).astype(F32)
    mine_first = first_of(reverse, core)
    first = jnp.where(mine_first, own[0:512].astype(F32), got[0:512].astype(F32))
    a_first = jnp.where(mine_first, decays_of(own[512:528]), decays_of(got[512:528]))
    after = first + per_row(a_first, 8) * before
    keep_ref[...] = jnp.where(mine_first, before, after).astype(BF)
    send_ref[...] = jnp.where(mine_first, after, before).astype(BF)


def along(distance, reverse):
    if reverse:
        return [(i, i - distance) for i in range(distance, 8)]
    return [(i, i + distance) for i in range(8 - distance)]


def scan(reverse, tag, sc, keep, send):
    swap = [(0, 1), (1, 0)]
    part = functools.partial
    half = sds((512, 128), BF)
    quarter, tailed = sds((256, 128), BF), sds((272, 128), BF)
    got = lax.ppermute(send, "c", swap)
    own_q, send_q = call_scratch(
        part(k_core, reverse), (tailed, tailed), "core" + tag, 1, (sc, keep, got), [pltpu.VMEM((2, 272, 128), BF)], 10**6
    )
    got_q = lax.ppermute(send_q, "xl", swap)
    plane = call(part(k_chip, reverse), tailed, "chip" + tag, 1, (sc, own_q, got_q), 10**6)
    near = lax.ppermute(plane, "z", along(1, reverse))
    far = lax.ppermute(plane, "z", along(2, reverse))
    two = call(k_two, quarter, "two" + tag, 1, (sc, near, far), 10**6)
    older = lax.ppermute(two, "z", along(2, reverse))
    keep_q, out_q = call(
        part(k_four, reverse), (quarter, quarter), "four" + tag, 1, (sc, near, far, two, older, own_q, got_q), 10**6
    )
    back_q = lax.ppermute(out_q, "xl", swap)
    keep_h, out_h = call_scratch(
        part(k_slab, reverse), (half, half), "slab" + tag, 1, (sc, keep_q, back_q, keep, got), [pltpu.VMEM((2, 256, 128), BF)], 10**6
    )
    back_h = lax.ppermute(out_h, "c", swap)
    return keep_h, back_h


def slab_out(reverse, tag, sc, skip, parts, b, c, values, state):
    cum, cum_t, dt_t, late = parts
    base = call_scratch(
        functools.partial(k_inside, reverse),
        sds((T, 1024), F32),
        "inside" + tag,
        2,
        (sc, skip, cum, cum_t, dt_t, b, c, values),
        [pltpu.VMEM((T, T), F32), pltpu.VMEM((T, T), F32)],
        10**9,
    )
    side = b if reverse else c
    return call_scratch(
        k_final,
        sds((T, 1024), BF),
        "final" + tag,
        1,
        (sc, base, late, side, state[0], state[1]),
        [pltpu.VMEM((2, 512, 128), BF)],
        10**7,
    )


def body(hidden, values, seg_next, proj_bc, proj_dt, dt_bias, decay, skip, bc_prev, dt_prev, seg_prev, grads):
    z, x, c = (lax.axis_index(n) for n in SEQ)
    k = lax.axis_index(FSDP)
    slab = lax.axis_index(SEQ)

    def scalars(lengths):
        b0 = lengths[0]
        b1 = b0 + lengths[1]
        b2 = b1 + lengths[2]
        return jnp.stack([b0, b1, b2, slab * T, c, x, z, k]).astype(jnp.int32)

    sc_next, sc_prev = scalars(seg_next), scalars(seg_prev)
    params = jnp.tile(lax.dynamic_slice_in_dim(jnp.stack([decay, dt_bias]), HEADS * k, HEADS, 1), (1, 8))

    weights = gather_weights(sc_next, proj_bc, proj_dt)

    group = k // 2
    b_prev = lax.dynamic_slice_in_dim(bc_prev, 128 * group, 128, 1)
    c_prev = lax.dynamic_slice_in_dim(bc_prev, 512 + 128 * group, 128, 1)
    dt_wide = jnp.tile(dt_prev, (1, 8))
    local = call_scratch(
        k_local_prev, LOCAL_OUTS, "local_prev", 1, (sc_prev, dt_wide, params, b_prev, c_prev, grads), [pltpu.VMEM((2, 528, 128), BF)], 10**8
    )
    state = scan(True, "_prev", sc_prev, local[0], local[1])
    grad_values = slab_out(True, "_prev", sc_prev, skip, local[2:6], b_prev, c_prev, grads, state)

    mine, dt_raw = call(k_project, (sds((T, 128), BF), sds((T, 128), F32)), "project", 1, (sc_next, hidden) + weights, 10**9)
    pair = lax.ppermute(mine, "y", [(i, i ^ 1) for i in range(4)])
    wide = sds((T, 128), BF)
    local = call_scratch(
        k_local_next, LOCAL_OUTS + (wide, wide), "local_next", 1, (sc_next, dt_raw, params, mine, pair, values), [pltpu.VMEM((2, 528, 128), BF)], 10**8
    )
    state = scan(False, "_next", sc_next, local[0], local[1])
    out_next = slab_out(False, "_next", sc_next, skip, local[2:6], local[6], local[7], values, state)
    return out_next, grad_values


def solution(mesh):
    split = Mesh(mesh.devices.reshape(8, 2, 2, 2, 4), ("z", "xl", "c", "xh", "y"))
    all_axes = SEQ + FSDP
    in_specs = (
        P(SEQ, None),
        P(SEQ, FSDP),
        P(),
        P(all_axes, None),
        P(all_axes, None),
        P(),
        P(),
        P(),
        P(SEQ, None),
        P(SEQ, FSDP),
        P(),
        P(SEQ, FSDP),
    )
    out_specs = (P(SEQ, FSDP), P(SEQ, FSDP))
    return jax.shard_map(body, mesh=split, in_specs=in_specs, out_specs=out_specs, check_vma=False)
```

```python
import functools
import jax
import jax.numpy as jnp
from jax import lax
from jax.experimental import pallas as pl
from jax.experimental.pallas import tpu as pltpu
from jax.sharding import Mesh
from jax.sharding import PartitionSpec as P

SEQ = ("z", "xl", "c")
FSDP = ("xh", "y")
BF = jnp.bfloat16
F32 = jnp.float32
T = 256
HEADS = 16
PAIRS = HEADS // 2
NEG = -1e30
VM = pl.BlockSpec(memory_space=pltpu.VMEM)
SM = pl.BlockSpec(memory_space=pltpu.SMEM)


def call(kernel, outs, name, n_smem, args, scratch=(), us=1, limit=12):
    return pl.pallas_call(
        kernel,
        out_shape=outs,
        in_specs=[SM] * n_smem + [VM] * (len(args) - n_smem),
        out_specs=jax.tree.map(lambda _: VM, outs),
        scratch_shapes=scratch,
        name=name,
        compiler_params=pltpu.CompilerParams(vmem_limit_bytes=limit << 20),
        cost_estimate=pl.CostEstimate(flops=us * 10_000_000, bytes_accessed=us * 100_000, transcendentals=0),
    )(*args)


def fsdp_place():
    return 4 * lax.axis_index("xh") + lax.axis_index("y")


def after(array, *others):
    return lax.optimization_barrier((array,) + others)[0]


def sds(shape, dtype):
    return jax.ShapeDtypeStruct(shape, dtype)


def lanes(shape):
    return lax.broadcasted_iota(jnp.int32, shape, len(shape) - 1)


def rows(shape):
    return lax.broadcasted_iota(jnp.int32, shape, len(shape) - 2)


def k_columns(bc_ref, dt_ref, out_ref):
    me = fsdp_place()
    lane = lanes((32, 128))
    low = lane < 64
    for j in range(4):
        b = bc_ref[:, 128 * j : 128 * j + 128].astype(F32)
        c = bc_ref[:, 512 + 128 * j : 640 + 128 * j].astype(F32)
        out_ref[2 * j, 0:32] = jnp.where(low, b, pltpu.roll(c, 64, 1)).astype(BF)
        out_ref[2 * j + 1, 0:32] = jnp.where(low, pltpu.roll(b, 64, 1), c).astype(BF)
    d = dt_ref[...].astype(F32)
    mine = lane // 16 == me
    for k in range(8):
        out_ref[k, 32:64] = jnp.where(mine, pltpu.roll(d, (16 * (me - k)) & 127, 1), 0.0).astype(BF)


def k_rows(rec_ref, out_ref):
    total = jnp.zeros((32, 128), F32)
    for k in range(8):
        out_ref[32 * k : 32 * k + 32] = rec_ref[k, 0:32]
        total = total + rec_ref[k, 32:64].astype(F32)
    out_ref[256:288] = total.astype(BF)


def k_quad(own, other_x, other_c, other_xc, out_ref):
    c, x = lax.axis_index("c"), lax.axis_index("xl")
    out_ref[2 * x + c] = own[...]
    out_ref[2 * (1 - x) + c] = other_x[...]
    out_ref[2 * x + 1 - c] = other_c[...]
    out_ref[2 * (1 - x) + 1 - c] = other_xc[...]


def weight_block(part):
    spread = (lanes((T, 128)) // 16) == (rows((T, 128)) // 32)
    packed = part[256:288]
    tall = jnp.concatenate([packed] * 8, axis=0)
    return jnp.concatenate([part[0:256], jnp.where(spread, tall, jnp.zeros_like(tall))], axis=1)


def times(hid, off, parts):
    left = hid[:, pl.ds(pl.multiple_of(off, 256), 256 * len(parts))]
    right = jnp.concatenate([weight_block(p) for p in parts], axis=0)
    return jnp.dot(left, right, preferred_element_type=F32)


def k_project_early(hid, q0, r1, g1, r2, g2, acc_ref):
    z, sign = lax.axis_index("z"), 1 - 2 * lax.axis_index("c")
    acc = times(hid, 1024 * z, [q0[b] for b in range(4)])
    for r, (up, down) in enumerate(((r1, g1), (r2, g2)), 1):
        acc = acc + times(hid, 1024 * ((z - sign * r) & 7), [up[b] for b in range(4)])
        acc = acc + times(hid, 1024 * ((z + sign * r) & 7), [down[b] for b in range(4)])
    acc_ref[...] = acc


def k_project_late(hid, early, r3, g3, h_own, h_other, y_ref, dt_ref):
    c, z = lax.axis_index("c"), lax.axis_index("z")
    sign = 1 - 2 * c
    acc = early[...] + times(hid, 1024 * ((z - sign * 3) & 7), [r3[b] for b in range(4)])
    acc = acc + times(hid, 1024 * ((z + sign * 3) & 7), [g3[b] for b in range(4)])
    far = 1024 * ((z + 4) & 7)
    acc = acc + times(hid, far + 512 * c, [h_own[b] for b in range(2)])
    acc = acc + times(hid, far + 512 * (1 - c), [h_other[b] for b in range(2)])
    y_ref[...] = acc[:, 0:128].astype(BF)
    d = acc[:, 128:256]
    for shift in (16, 32, 64):
        d = d + pltpu.roll(d, shift, 1)
    dt_ref[...] = d


def slab_start():
    return T * (4 * lax.axis_index("z") + 2 * lax.axis_index("xl") + lax.axis_index("c"))


def bounds_of(lengths):
    b0 = lengths[0]
    b1 = b0 + lengths[1]
    return b0, b1, b1 + lengths[2]


def segment_of(lengths, places):
    one, none = jnp.int32(1), jnp.int32(0)
    return sum((jnp.where(places >= b, one, none) for b in bounds_of(lengths)), none)


def expand(factor, j, low):
    a = jnp.broadcast_to(factor[:, 2 * j : 2 * j + 1], (T, 128))
    b = jnp.broadcast_to(factor[:, 2 * j + 1 : 2 * j + 2], (T, 128))
    return jnp.where(low, a, b)


def head_lanes(row):
    r = pltpu.roll(jnp.broadcast_to(row, (8, 128)), (128 - HEADS * fsdp_place()) & 127, 1)
    r = jnp.where(lanes((8, 128)) < HEADS, r, 0.0)
    for shift in (16, 32, 64):
        r = r + pltpu.roll(r, shift, 1)
    return r[0:1]


def local_part(reverse, sc, dt, dt_t, decay_row, b, c, val_ref, outs, scratch):
    keep_ref, send_ref, cum_ref, cumt_ref, dtt_ref, late_ref = outs
    offset, core = slab_start(), lax.axis_index("c")
    decay = head_lanes(decay_row)
    before, last = segment_of(sc, offset - 1), segment_of(sc, offset + T - 1)
    x = -jnp.transpose(dt * decay)[0:HEADS]
    lane = lanes((HEADS, T))
    for shift in (1, 2, 4, 8, 16, 32, 64, 128):
        x = x + jnp.where(lane >= shift, pltpu.roll(x, shift, 1), 0.0)
    cum_t = x
    cum = jnp.transpose(jnp.concatenate([cum_t] * 8, axis=0))
    final = cum[T - 1 : T]
    place = offset + rows((T, 128))
    seg = segment_of(sc, place)
    send = jnp.where(seg == last, jnp.exp(final - cum) * dt, 0.0)
    read = jnp.where(seg == before, jnp.exp(cum), 0.0)
    early, late = (read, send) if reverse else (send, read)
    cum_ref[...] = cum
    cumt_ref[...] = cum_t
    dtt_ref[...] = dt_t
    late_ref[...] = late
    low = lanes((T, 128)) < 64
    side = c if reverse else b
    for j in range(PAIRS):
        v = val_ref[:, 128 * j : 128 * j + 128].astype(F32)
        scaled = (v * expand(early, j, low)).astype(BF)
        out = lax.dot_general(scaled, side, (((0,), (0,)), ((), ())), preferred_element_type=F32)
        scratch[j // 4, 128 * (j % 4) : 128 * (j % 4) + 128] = out
    a = jnp.broadcast_to(jnp.exp(cum_t[:, T - 1 : T]), (HEADS, 128))
    a = jnp.where(last == before, a, 0.0)
    high = a.astype(BF).astype(F32)
    rest = a - high
    for half in range(2):
        pick = slice(8 * half, 8 * half + 8)
        scratch[half, 512:528] = jnp.concatenate([high[pick], rest[pick]], axis=0)
    keep_ref[...] = scratch[core]
    send_ref[...] = scratch[1 - core].astype(BF)


def group_columns(bc_ref, first):
    at = first + 128 * (fsdp_place() // 2)
    return bc_ref[:, pl.ds(pl.multiple_of(at, 128), 128)]


def k_local_prev(sc, dtt_ref, decay_ref, bc_ref, val_ref, *refs):
    dt_t = dtt_ref[...]
    dt = jnp.transpose(jnp.concatenate([dt_t] * 8, axis=0))
    local_part(True, sc, dt, dt_t, decay_ref[...], group_columns(bc_ref, 0), group_columns(bc_ref, 512), val_ref, refs[:6], refs[6])


def softplus(v):
    return jnp.maximum(v, 0.0) + jnp.log1p(jnp.exp(-jnp.abs(v)))


def k_local_next(sc, dt_ref, decay_ref, bias_ref, mine_ref, pair_ref, val_ref, *refs):
    outs, b_out, c_out, scratch = refs[:6], refs[6], refs[7], refs[8]
    odd = (lax.axis_index("y") & 1) == 1
    mine, pair = mine_ref[...].astype(F32), pair_ref[...].astype(F32)
    lo, hi = jnp.where(odd, pair, mine), jnp.where(odd, mine, pair)
    low = lanes((T, 128)) < 64
    b = jnp.where(low, lo, pltpu.roll(hi, 64, 1)).astype(BF)
    c = jnp.where(low, pltpu.roll(lo, 64, 1), hi).astype(BF)
    b_out[...] = b
    c_out[...] = c
    dt = softplus(dt_ref[...] + head_lanes(bias_ref[...]))
    local_part(False, sc, dt, jnp.transpose(dt)[0:HEADS], decay_ref[...], b, c, val_ref, outs, scratch)


LOCAL_OUTS = (
    sds((528, 128), F32),
    sds((528, 128), BF),
    sds((T, 128), F32),
    sds((HEADS, T), F32),
    sds((HEADS, T), F32),
    sds((T, 128), F32),
)


def sides(reverse, refs):
    if reverse:
        return group_columns(refs[0], 0), group_columns(refs[0], 512)
    return refs[0][...], refs[1][...]


def k_inside(reverse, sc, skip, cum_ref, cumt_ref, dtt_ref, val_ref, *refs):
    out_ref, bias_ref, score_ref = refs[-3:]
    offset, first_head = slab_start(), HEADS * fsdp_place()
    shape = (T, T)
    seg_r = segment_of(sc, offset + rows(shape))
    seg_l = segment_of(sc, offset + lanes(shape))
    causal = rows(shape) <= lanes(shape) if reverse else rows(shape) >= lanes(shape)
    bias_ref[...] = jnp.where((seg_r == seg_l) & causal, 0.0, NEG)
    b, c = sides(reverse, refs)
    one, two = (b, c) if reverse else (c, b)
    score_ref[...] = lax.dot_general(one, two, (((1,), (1,)), ((), ())), preferred_element_type=F32)
    low = lanes((T, 128)) < 64
    cum = cum_ref[...]
    for j in range(PAIRS):
        v = val_ref[:, 128 * j : 128 * j + 128]
        parts = []
        for h in (2 * j, 2 * j + 1):
            col = jnp.broadcast_to(cum[:, h : h + 1], shape)
            row = cumt_ref[h : h + 1]
            if reverse:
                spread = row - col
            else:
                spread = col - row
            decays = jnp.exp(spread + bias_ref[...])
            if reverse:
                mix = (decays * score_ref[...])
            else:
                mix = decays * dtt_ref[h : h + 1] * score_ref[...]
            parts.append(jnp.dot(mix.astype(BF), v, preferred_element_type=F32))
        inside = jnp.where(low, parts[0], parts[1])
        gain = jnp.where(low, skip[first_head + 2 * j], skip[first_head + 2 * j + 1])
        if reverse:
            dt = jnp.transpose(jnp.concatenate([dtt_ref[...]] * 8, axis=0)) if j == 0 else dt
            inside = inside * expand(dt, j, low)
        out_ref[:, 128 * j : 128 * j + 128] = inside + gain * v.astype(F32)


def k_final(reverse, base_ref, late_ref, keep_ref, got_ref, *refs):
    out_ref, scratch = refs[-2:]
    core = lax.axis_index("c")
    scratch[core] = keep_ref[...].astype(BF)
    scratch[1 - core] = got_ref[...]
    low = lanes((T, 128)) < 64
    late = late_ref[...]
    b, c = sides(reverse, refs)
    side = b if reverse else c
    for j in range(PAIRS):
        st = scratch[j // 4, 128 * (j % 4) : 128 * (j % 4) + 128]
        seen = lax.dot_general(side, st, (((1,), (1,)), ((), ())), preferred_element_type=F32)
        at = slice(128 * j, 128 * j + 128)
        out_ref[:, at] = (base_ref[:, at] + expand(late, j, low) * seen).astype(BF)


def decays_of(tail):
    t = tail.astype(F32)
    return t[0:8] + t[8:16]


def tail_of(a):
    high = a.astype(BF).astype(F32)
    return jnp.concatenate([high, a - high], axis=0)


def per_row(a, heads):
    return jnp.concatenate([jnp.broadcast_to(a[h : h + 1], (64, 128)) for h in range(heads)], axis=0)


def quarter_rows(a, which):
    return per_row(jnp.where(which == 0, a[0:4], a[4:8]), 4)


def first_of(reverse, bit):
    return (bit == 1) if reverse else (bit == 0)


def k_core(reverse, own, got, keep_ref, send_ref, scratch):
    core, x = lax.axis_index("c"), lax.axis_index("xl")
    mine_first = first_of(reverse, core)
    so, sg = own[0:512], got[0:512].astype(F32)
    ao, ag = decays_of(own[512:528]), decays_of(got[512:528])
    first, second = jnp.where(mine_first, so, sg), jnp.where(mine_first, sg, so)
    a_second = jnp.where(mine_first, ag, ao)
    joined = second + per_row(a_second, 8) * first
    tail = tail_of(ao * ag)
    for q in range(2):
        scratch[q, 0:256] = joined[256 * q : 256 * q + 256]
        scratch[q, 256:272] = tail
    keep_ref[...] = scratch[x]
    send_ref[...] = scratch[1 - x].astype(BF)


def k_chip(reverse, own, got, out_ref):
    x = lax.axis_index("xl")
    mine_first = first_of(reverse, x)
    so, sg = own[0:256], got[0:256].astype(F32)
    ao, ag = decays_of(own[256:272]), decays_of(got[256:272])
    first, second = jnp.where(mine_first, so, sg), jnp.where(mine_first, sg, so)
    a_second = jnp.where(mine_first, ag, ao)
    out_ref[0:256] = (second + quarter_rows(a_second, x) * first).astype(BF)
    out_ref[256:272] = tail_of(ao * ag).astype(BF)


def k_two(near, far, keep_ref, send_ref):
    x = lax.axis_index("xl")
    a = decays_of(near[256:272])
    two = near[0:256].astype(F32) + quarter_rows(a, x) * far[0:256].astype(F32)
    keep_ref[...] = two
    send_ref[...] = two.astype(BF)


def k_four(reverse, near, far, pair, older, own, got, keep_ref, send_ref):
    x = lax.axis_index("xl")
    a = decays_of(near[256:272]) * decays_of(far[256:272])
    before = pair[...] + quarter_rows(a, x) * older[...].astype(F32)
    mine_first = first_of(reverse, x)
    first = jnp.where(mine_first, own[0:256], got[0:256].astype(F32))
    a_first = jnp.where(mine_first, decays_of(own[256:272]), decays_of(got[256:272]))
    after = first + quarter_rows(a_first, x) * before
    keep_ref[...] = jnp.where(mine_first, before, after)
    send_ref[...] = jnp.where(mine_first, after, before).astype(BF)


def k_slab(reverse, mine, other, own, got, keep_ref, send_ref, scratch):
    core, x = lax.axis_index("c"), lax.axis_index("xl")
    scratch[x] = mine[...]
    scratch[1 - x] = other[...].astype(F32)
    before = jnp.concatenate([scratch[0], scratch[1]], axis=0)
    mine_first = first_of(reverse, core)
    first = jnp.where(mine_first, own[0:512], got[0:512].astype(F32))
    a_first = jnp.where(mine_first, decays_of(own[512:528]), decays_of(got[512:528]))
    after = first + per_row(a_first, 8) * before
    keep_ref[...] = jnp.where(mine_first, before, after)
    send_ref[...] = jnp.where(mine_first, after, before).astype(BF)


def along(distance, reverse):
    if reverse:
        return [(i, i - distance) for i in range(distance, 8)]
    return [(i, i + distance) for i in range(8 - distance)]


SWAP = [(0, 1), (1, 0)]
HALF, QUARTER, TAILED = (512, 128), (256, 128), (272, 128)


def both(shape):
    return sds(shape, F32), sds(shape, BF)


class Scan:
    def __init__(self, reverse, tag, keep, send):
        self.reverse, self.tag, self.keep, self.send = reverse, tag, keep, send

    def run(self, kernel, outs, name, args, scratch=()):
        return call(functools.partial(kernel, self.reverse), outs, name + self.tag, 0, args, scratch)

    def core(self):
        self.got = lax.ppermute(self.send, "c", SWAP)
        self.own_q, self.send_q = self.run(k_core, both(TAILED), "core", (self.keep, self.got), [pltpu.VMEM((2,) + TAILED, F32)])
        return self.send_q

    def chip(self):
        self.got_q = lax.ppermute(self.send_q, "xl", SWAP)
        self.plane = self.run(k_chip, sds(TAILED, BF), "chip", (self.own_q, self.got_q))
        return self.plane

    def two(self):
        self.near = lax.ppermute(self.plane, "z", along(1, self.reverse))
        self.far = lax.ppermute(self.plane, "z", along(2, self.reverse))
        self.pair, self.pair_send = call(k_two, both(QUARTER), "two" + self.tag, 0, (self.near, self.far))
        return self.pair_send

    def four(self):
        older = lax.ppermute(self.pair_send, "z", along(2, self.reverse))
        args = (self.near, self.far, self.pair, older, self.own_q, self.got_q)
        self.keep_q, self.out_q = self.run(k_four, both(QUARTER), "four", args)
        return self.out_q

    def slab(self):
        back = lax.ppermute(self.out_q, "xl", SWAP)
        args = (self.keep_q, back, self.keep, self.got)
        self.keep_h, self.out_h = self.run(k_slab, both(HALF), "slab", args, [pltpu.VMEM((2,) + QUARTER, F32)])
        return self.out_h

    def state(self):
        return self.keep_h, lax.ppermute(self.out_h, "c", SWAP)


def inside(reverse, tag, lengths, skip, parts, values, bc):
    cum, cum_t, dt_t, _ = parts
    args = (lengths, skip, cum, cum_t, dt_t, values) + bc
    scratch = [pltpu.VMEM((T, T), F32), pltpu.VMEM((T, T), F32)]
    return call(functools.partial(k_inside, reverse), sds((T, 1024), F32), "inside" + tag, 2, args, scratch, us=3)


def final(reverse, tag, base, late, state, bc):
    args = (base, late) + tuple(state) + bc
    kernel = functools.partial(k_final, reverse)
    return call(kernel, sds((T, 1024), BF), "final" + tag, 0, args, [pltpu.VMEM((2, 512, 128), BF)], us=2)


def body(hidden, values, seg_next, proj_bc, proj_dt, dt_bias, decay, skip, bc_prev, dt_prev, seg_prev, grads):
    decay_row, bias_row = decay[None, :], dt_bias[None, :]
    wide = sds((T, 128), BF)

    send = call(k_columns, sds((8, 64, 128), BF), "columns", 0, (proj_bc, proj_dt))
    got = lax.all_to_all(send, FSDP, 0, 0, tiled=False)
    own = call(k_rows, sds((288, 128), BF), "rows", 0, (got,))

    other_x = lax.ppermute(own, "xl", SWAP)
    other_c = lax.ppermute(own, "c", SWAP)
    other_xc = lax.ppermute(other_x, "c", SWAP)
    args = (after(seg_prev, own), dt_prev.T, decay_row, bc_prev, grads)
    local = call(k_local_prev, LOCAL_OUTS, "local_prev", 1, args, [pltpu.VMEM((2, 528, 128), F32)], us=3)
    prev = Scan(True, "_prev", local[0], local[1])
    parts_prev = local[2:6]
    q0 = call(k_quad, sds((4, 288, 128), BF), "quad", 0, (own, other_x, other_c, after(other_xc, local[1])))

    ring = [(2 * z, 2 * ((z + 1) % 8)) for z in range(8)] + [(2 * z + 1, 2 * ((z - 1) % 8) + 1) for z in range(8)]
    r1 = lax.ppermute(q0, ("z", "c"), ring)
    step = prev.core()
    r1 = after(r1, step)
    r2 = lax.ppermute(r1, ("z", "c"), ring)
    g1 = lax.ppermute(r1, "c", SWAP)
    step = prev.chip()
    r2 = after(r2, step, g1)
    r3 = lax.ppermute(r2, ("z", "c"), ring)
    g2 = lax.ppermute(r2, "c", SWAP)
    early = call(k_project_early, sds((T, 256), F32), "project_early", 0, (hidden, q0, r1, g1, r2, g2), us=3, limit=20)
    r3 = after(r3, early)
    half = lax.dynamic_slice_in_dim(r3, 2 * lax.axis_index("c"), 2, 0)
    h_own = lax.ppermute(half, ("z", "c"), ring)
    g3 = lax.ppermute(r3, "c", SWAP)
    step = prev.two()
    h_own = after(h_own, g3, step)
    h_other = lax.ppermute(h_own, "c", SWAP)
    mine, dt_raw = call(
        k_project_late, (wide, sds((T, 128), F32)), "project_late", 0, (hidden, early, r3, g3, h_own, h_other), us=2, limit=20
    )

    pair = lax.ppermute(mine, "y", [(i, i ^ 1) for i in range(4)])
    step = prev.four()
    pair = after(pair, step)
    args = (seg_next, dt_raw, decay_row, bias_row, mine, pair, values)
    local = call(k_local_next, LOCAL_OUTS + (wide, wide), "local_next", 1, args, [pltpu.VMEM((2, 528, 128), F32)], us=3)
    nxt = Scan(False, "_next", local[0], local[1])
    parts_next, bc_next = local[2:6], (local[6], local[7])
    nxt.core()
    base_next = inside(False, "_next", seg_next, skip, parts_next, values, bc_next)
    nxt.send_q = after(nxt.send_q, step)
    nxt.chip()
    step = prev.slab()
    nxt.plane = after(nxt.plane, base_next)
    nxt.two()
    base_prev = inside(True, "_prev", seg_prev, skip, parts_prev, grads, (bc_prev,))
    state_prev = prev.state()
    nxt.pair_send = after(nxt.pair_send, step, base_prev)
    nxt.four()
    nxt.out_q = after(nxt.out_q, state_prev[1])
    grad_values = final(True, "_prev", base_prev, parts_prev[3], state_prev, (bc_prev,))
    nxt.slab()
    nxt.out_h = after(nxt.out_h, grad_values)
    out_next = final(False, "_next", base_next, parts_next[3], nxt.state(), bc_next)
    return out_next, grad_values


def solution(mesh):
    split = Mesh(mesh.devices.reshape(8, 2, 2, 2, 4), ("z", "xl", "c", "xh", "y"))
    all_axes = SEQ + FSDP
    in_specs = (
        P(SEQ, None),
        P(SEQ, FSDP),
        P(),
        P(all_axes, None),
        P(all_axes, None),
        P(),
        P(),
        P(),
        P(SEQ, None),
        P(SEQ, FSDP),
        P(),
        P(SEQ, FSDP),
    )
    out_specs = (P(SEQ, FSDP), P(SEQ, FSDP))
    return jax.shard_map(body, mesh=split, in_specs=in_specs, out_specs=out_specs, check_vma=False)
```

```python
import functools
import jax
import jax.numpy as jnp
from jax import lax
from jax.experimental import pallas as pl
from jax.experimental.pallas import tpu as pltpu
from jax.sharding import Mesh
from jax.sharding import PartitionSpec as P

SEQ = ("z", "xl", "c")
FSDP = ("xh", "y")
BF = jnp.bfloat16
F32 = jnp.float32
T = 256
HEADS = 16
PAIRS = HEADS // 2
NEG = -1e30
VM = pl.BlockSpec(memory_space=pltpu.VMEM)
SM = pl.BlockSpec(memory_space=pltpu.SMEM)


def call(kernel, outs, name, n_smem, args, scratch=(), us=1, limit=12):
    return pl.pallas_call(
        kernel,
        out_shape=outs,
        in_specs=[SM] * n_smem + [VM] * (len(args) - n_smem),
        out_specs=jax.tree.map(lambda _: VM, outs),
        scratch_shapes=scratch,
        name=name,
        compiler_params=pltpu.CompilerParams(vmem_limit_bytes=limit << 20),
        cost_estimate=pl.CostEstimate(flops=us * 10_000_000, bytes_accessed=us * 100_000, transcendentals=0),
    )(*args)


def fsdp_place():
    return 4 * lax.axis_index("xh") + lax.axis_index("y")


def after(array, *others):
    return lax.optimization_barrier((array,) + others)[0]


def sds(shape, dtype):
    return jax.ShapeDtypeStruct(shape, dtype)


def lanes(shape):
    return lax.broadcasted_iota(jnp.int32, shape, len(shape) - 1)


def rows(shape):
    return lax.broadcasted_iota(jnp.int32, shape, len(shape) - 2)


def k_columns(bc_ref, dt_ref, out_ref):
    low = lanes((32, 128)) < 64
    parts = []
    for j in range(4):
        b = bc_ref[:, 128 * j : 128 * j + 128].astype(F32)
        c = bc_ref[:, 512 + 128 * j : 640 + 128 * j].astype(F32)
        parts.append(jnp.where(low, b, pltpu.roll(c, 64, 1)))
        parts.append(jnp.where(low, pltpu.roll(b, 64, 1), c))
    d = dt_ref[...].astype(F32)
    diagonal = lanes((8, 128)) // 16 == rows((8, 128))
    for k in range(8):
        packed = []
        for q in range(4):
            piece = jnp.concatenate(
                [pltpu.roll(d[8 * q : 8 * q + 8], (16 * (i - k)) % 128, 1)[i : i + 1] for i in range(8)], axis=0
            )
            packed.append(jnp.sum(jnp.where(diagonal, piece, 0.0), axis=0, keepdims=True))
        whole = jnp.concatenate([parts[k]] + packed + [jnp.zeros((4, 128), F32)], axis=0)[0:36].astype(BF)
        for x in range(2):
            out_ref[x, k] = whole


def k_rows(rec_ref, out_ref):
    group = lanes((8, 128)) // 16
    sub = rows((8, 128))
    for x in range(2):
        for m in range(8):
            out_ref[x, 32 * m : 32 * m + 32] = rec_ref[8 * x + m, 0:32]
        tails = [rec_ref[8 * x + m, 32:36].astype(F32) for m in range(8)]
        done = []
        for q in range(4):
            a = jnp.concatenate([t[q : q + 1] for t in tails], axis=0)
            out = jnp.zeros((8, 128), F32)
            for d in range(8):
                moved = pltpu.roll(pltpu.roll(a, (8 - d) % 8, 0), 16 * d, 1)
                out = jnp.where(group == ((sub + d) & 7), moved, out)
            done.append(out)
        out_ref[x, 256:288] = jnp.concatenate(done, axis=0).astype(BF)


def k_pack(a, b, out_ref):
    out_ref[0:2] = a[...]
    out_ref[2:4] = b[...]


def k_load(hid_ref, out_ref):
    pltpu.sync_copy(hid_ref, out_ref)


def weight_block(part):
    spread = (lanes((T, 128)) // 16) == (rows((T, 128)) // 32)
    packed = part[256:288]
    tall = jnp.concatenate([packed] * 8, axis=0)
    return jnp.concatenate([part[0:256], jnp.where(spread, tall, jnp.zeros_like(tall))], axis=1)


def side_of_pair():
    return 1 - 2 * ((lax.axis_index("z") + lax.axis_index("c")) & 1)


def times(hid, parts, planes, core):
    left = [
        hid[:, pl.ds(pl.multiple_of(1024 * (p & 7) + 512 * x + 256 * core, 256), 256)] for p in planes for x in range(2)
    ]
    right = jnp.concatenate([weight_block(parts[b]) for b in range(4)], axis=0)
    return jnp.dot(jnp.concatenate(left, axis=1), right, preferred_element_type=F32)


def k_project(step, last, *refs):
    hid, refs = refs[0], refs[1:]
    z, c, s = lax.axis_index("z"), lax.axis_index("c"), side_of_pair()
    acc = None if step[0] == 0 else refs[0][...]
    if step[0] > 0:
        refs = refs[1:]
    for n, at in enumerate(step):
        first, second = ((0, 1), (-1, -2), (2, 3), (-3, -4))[at]
        mine = times(hid, refs[2 * n], (z + s * first, z + s * second), c)
        acc = mine if acc is None else acc + mine
        acc = acc + times(hid, refs[2 * n + 1], (z - s * first, z - s * second), 1 - c)
    if not last:
        refs[-1][...] = acc
        return
    y_ref, dt_ref = refs[-2:]
    y_ref[...] = acc[:, 0:128].astype(BF)
    d = acc[:, 128:256]
    for shift in (16, 32, 64):
        d = d + pltpu.roll(d, shift, 1)
    dt_ref[...] = d


def slab_start():
    return T * (4 * lax.axis_index("z") + 2 * lax.axis_index("xl") + lax.axis_index("c"))


def bounds_of(lengths):
    b0 = lengths[0]
    b1 = b0 + lengths[1]
    return b0, b1, b1 + lengths[2]


def segment_of(lengths, places):
    one, none = jnp.int32(1), jnp.int32(0)
    return sum((jnp.where(places >= b, one, none) for b in bounds_of(lengths)), none)


def expand(factor, j, low):
    a = jnp.broadcast_to(factor[:, 2 * j : 2 * j + 1], (T, 128))
    b = jnp.broadcast_to(factor[:, 2 * j + 1 : 2 * j + 2], (T, 128))
    return jnp.where(low, a, b)


def head_lanes(row):
    r = pltpu.roll(jnp.broadcast_to(row, (8, 128)), (128 - HEADS * fsdp_place()) & 127, 1)
    r = jnp.where(lanes((8, 128)) < HEADS, r, 0.0)
    for shift in (16, 32, 64):
        r = r + pltpu.roll(r, shift, 1)
    return r[0:1]


def local_part(reverse, sc, dt, dt_t, decay_row, b, c, val_ref, outs, scratch):
    keep_ref, send_ref, cum_ref, cumt_ref, dtt_ref, late_ref = outs
    offset, core = slab_start(), lax.axis_index("c")
    decay = head_lanes(decay_row)
    before, last = segment_of(sc, offset - 1), segment_of(sc, offset + T - 1)
    x = -jnp.transpose(dt * decay)[0:HEADS]
    lane = lanes((HEADS, T))
    for shift in (1, 2, 4, 8, 16, 32, 64, 128):
        x = x + jnp.where(lane >= shift, pltpu.roll(x, shift, 1), 0.0)
    cum_t = x
    cum = jnp.transpose(jnp.concatenate([cum_t] * 8, axis=0))
    final = cum[T - 1 : T]
    place = offset + rows((T, 128))
    seg = segment_of(sc, place)
    send = jnp.where(seg == last, jnp.exp(final - cum) * dt, 0.0)
    read = jnp.where(seg == before, jnp.exp(cum), 0.0)
    early, late = (read, send) if reverse else (send, read)
    cum_ref[...] = cum
    cumt_ref[...] = cum_t
    dtt_ref[...] = dt_t
    late_ref[...] = late
    low = lanes((T, 128)) < 64
    side = c if reverse else b
    for j in range(PAIRS):
        v = val_ref[:, 128 * j : 128 * j + 128].astype(F32)
        scaled = (v * expand(early, j, low)).astype(BF)
        out = lax.dot_general(scaled, side, (((0,), (0,)), ((), ())), preferred_element_type=F32)
        scratch[j // 4, 128 * (j % 4) : 128 * (j % 4) + 128] = out
    a = jnp.broadcast_to(jnp.exp(cum_t[:, T - 1 : T]), (HEADS, 128))
    a = jnp.where(last == before, a, 0.0)
    high = a.astype(BF).astype(F32)
    rest = a - high
    for half in range(2):
        pick = slice(8 * half, 8 * half + 8)
        scratch[half, 512:528] = jnp.concatenate([high[pick], rest[pick]], axis=0)
    keep_ref[...] = scratch[core]
    send_ref[...] = scratch[1 - core].astype(BF)


def group_columns(bc_ref, first):
    at = first + 128 * (fsdp_place() // 2)
    return bc_ref[:, pl.ds(pl.multiple_of(at, 128), 128)]


def k_local_prev(sc, dtt_ref, decay_ref, bc_ref, val_ref, *refs):
    dt_t = dtt_ref[...]
    dt = jnp.transpose(jnp.concatenate([dt_t] * 8, axis=0))
    local_part(True, sc, dt, dt_t, decay_ref[...], group_columns(bc_ref, 0), group_columns(bc_ref, 512), val_ref, refs[:6], refs[6])


def softplus(v):
    return jnp.maximum(v, 0.0) + jnp.log1p(jnp.exp(-jnp.abs(v)))


def k_local_next(sc, dt_ref, decay_ref, bias_ref, mine_ref, pair_ref, val_ref, *refs):
    outs, b_out, c_out, scratch = refs[:6], refs[6], refs[7], refs[8]
    odd = (lax.axis_index("y") & 1) == 1
    mine, pair = mine_ref[...].astype(F32), pair_ref[...].astype(F32)
    lo, hi = jnp.where(odd, pair, mine), jnp.where(odd, mine, pair)
    low = lanes((T, 128)) < 64
    b = jnp.where(low, lo, pltpu.roll(hi, 64, 1)).astype(BF)
    c = jnp.where(low, pltpu.roll(lo, 64, 1), hi).astype(BF)
    b_out[...] = b
    c_out[...] = c
    dt = softplus(dt_ref[...] + head_lanes(bias_ref[...]))
    local_part(False, sc, dt, jnp.transpose(dt)[0:HEADS], decay_ref[...], b, c, val_ref, outs, scratch)


LOCAL_OUTS = (
    sds((528, 128), F32),
    sds((528, 128), BF),
    sds((T, 128), F32),
    sds((HEADS, T), F32),
    sds((HEADS, T), F32),
    sds((T, 128), F32),
)


def sides(reverse, refs):
    if reverse:
        return group_columns(refs[0], 0), group_columns(refs[0], 512)
    return refs[0][...], refs[1][...]


def k_inside(reverse, sc, skip, cum_ref, cumt_ref, dtt_ref, val_ref, *refs):
    out_ref, bias_ref, score_ref = refs[-3:]
    offset, first_head = slab_start(), HEADS * fsdp_place()
    shape = (T, T)
    seg_r = segment_of(sc, offset + rows(shape))
    seg_l = segment_of(sc, offset + lanes(shape))
    causal = rows(shape) <= lanes(shape) if reverse else rows(shape) >= lanes(shape)
    bias_ref[...] = jnp.where((seg_r == seg_l) & causal, 0.0, NEG)
    b, c = sides(reverse, refs)
    one, two = (b, c) if reverse else (c, b)
    score_ref[...] = lax.dot_general(one, two, (((1,), (1,)), ((), ())), preferred_element_type=F32)
    low = lanes((T, 128)) < 64
    cum = cum_ref[...]
    for j in range(PAIRS):
        v = val_ref[:, 128 * j : 128 * j + 128]
        parts = []
        for h in (2 * j, 2 * j + 1):
            col = jnp.broadcast_to(cum[:, h : h + 1], shape)
            row = cumt_ref[h : h + 1]
            if reverse:
                spread = row - col
            else:
                spread = col - row
            decays = jnp.exp(spread + bias_ref[...])
            if reverse:
                mix = (decays * score_ref[...])
            else:
                mix = decays * dtt_ref[h : h + 1] * score_ref[...]
            parts.append(jnp.dot(mix.astype(BF), v, preferred_element_type=F32))
        inside = jnp.where(low, parts[0], parts[1])
        gain = jnp.where(low, skip[first_head + 2 * j], skip[first_head + 2 * j + 1])
        if reverse:
            dt = jnp.transpose(jnp.concatenate([dtt_ref[...]] * 8, axis=0)) if j == 0 else dt
            inside = inside * expand(dt, j, low)
        out_ref[:, 128 * j : 128 * j + 128] = inside + gain * v.astype(F32)


def k_final(reverse, base_ref, late_ref, keep_ref, got_ref, *refs):
    out_ref, scratch = refs[-2:]
    core, r = lax.axis_index("c"), int(reverse)
    scratch[core] = keep_ref[r]
    scratch[1 - core] = got_ref[r]
    low = lanes((T, 128)) < 64
    late = late_ref[...]
    b, c = sides(reverse, refs)
    side = b if reverse else c
    for j in range(PAIRS):
        st = scratch[j // 4, 128 * (j % 4) : 128 * (j % 4) + 128]
        seen = lax.dot_general(side, st, (((1,), (1,)), ((), ())), preferred_element_type=F32)
        at = slice(128 * j, 128 * j + 128)
        out_ref[:, at] = (base_ref[:, at] + expand(late, j, low) * seen).astype(BF)


def decays_of(tail):
    t = tail.astype(F32)
    return t[0:8] + t[8:16]


def tail_of(a):
    high = a.astype(BF).astype(F32)
    return jnp.concatenate([high, a - high], axis=0)


def per_row(a, heads):
    return jnp.concatenate([jnp.broadcast_to(a[h : h + 1], (64, 128)) for h in range(heads)], axis=0)


def quarter_rows(a, which):
    return per_row(jnp.where(which == 0, a[0:4], a[4:8]), 4)


def first_of(reverse, bit):
    return (bit == 1) if reverse else (bit == 0)


def k_core(reverse, own, got, keep_ref, send_ref, scratch):
    core, x = lax.axis_index("c"), lax.axis_index("xl")
    mine_first = first_of(reverse, core)
    so, sg = own[0:512], got[0:512].astype(F32)
    ao, ag = decays_of(own[512:528]), decays_of(got[512:528])
    first, second = jnp.where(mine_first, so, sg), jnp.where(mine_first, sg, so)
    a_second = jnp.where(mine_first, ag, ao)
    joined = second + per_row(a_second, 8) * first
    tail = tail_of(ao * ag)
    for q in range(2):
        scratch[q, 0:256] = joined[256 * q : 256 * q + 256]
        scratch[q, 256:272] = tail
    keep_ref[...] = scratch[x]
    send_ref[...] = scratch[1 - x].astype(BF)


def chip_sum(reverse, own, got):
    x = lax.axis_index("xl")
    mine_first = first_of(reverse, x)
    so, sg = own[0:256], got[0:256].astype(F32)
    ao, ag = decays_of(own[256:272]), decays_of(got[256:272])
    first, second = jnp.where(mine_first, so, sg), jnp.where(mine_first, sg, so)
    a_second = jnp.where(mine_first, ag, ao)
    return second + quarter_rows(a_second, x) * first, tail_of(ao * ag)


def k_chip_prev(own, got, out_ref):
    out_ref[0:256], out_ref[256:272] = chip_sum(True, own, got)


def k_chip_next(own, got, prev, out_ref, msg_ref):
    state, tail = chip_sum(False, own, got)
    out_ref[0:256], out_ref[256:272] = state, tail
    msg_ref[0, 0:256], msg_ref[0, 256:272] = state.astype(BF), tail.astype(BF)
    msg_ref[1] = prev[...].astype(BF)


def pair_place():
    z, c = lax.axis_index("z"), lax.axis_index("c")
    q = z + c
    alone = (c == 1) & ((z == 0) | (z == 7))
    return q // 2, (q & 1) == 1, jnp.logical_not(alone), 3 + c


def k_pairs(next_ref, prev_ref, got, out_ref):
    x = lax.axis_index("xl")
    _, upper, partner, _ = pair_place()
    sums = []
    for r, own in enumerate((next_ref, prev_ref)):
        mine_first = jnp.logical_not(upper) if r == 0 else upper
        so, ao = own[0:256], decays_of(own[256:272])
        sg, ag = got[r, 0:256].astype(F32), decays_of(got[r, 256:272])
        first, second = jnp.where(mine_first, so, sg), jnp.where(mine_first, sg, so)
        total = second + quarter_rows(jnp.where(mine_first, ag, ao), x) * first
        sums.append((jnp.where(partner, total, so), tail_of(jnp.where(partner, ao * ag, ao))))
    out_ref[0:256] = jnp.where(upper, sums[0][0], sums[1][0]).astype(BF)
    out_ref[256:272] = jnp.where(upper, sums[0][1], sums[1][1]).astype(BF)


def k_planes(got, m2, m3, m4, m5, own_n, got_n, own_p, got_p, keep_ref, send_ref):
    x = lax.axis_index("xl")
    m, upper, partner, top = pair_place()
    for r, (own, other) in enumerate(((own_n, got_n), (own_p, got_p))):
        straight = upper if r == 1 else jnp.logical_not(upper)
        near_there = (m + 1 <= top) if r == 1 else (m >= 1)
        far_there = (m + 2 <= top) if r == 1 else (m >= 2)
        near = jnp.where(straight, m2[...].astype(F32), m3[...].astype(F32))
        far = jnp.where(straight, m4[0:256].astype(F32), m5[0:256].astype(F32))
        far = jnp.where(far_there, far, 0.0)
        total = near[0:256] + quarter_rows(near[256:264] + near[264:272], x) * far
        total = jnp.where(near_there, total, 0.0)
        beyond = got[r, 0:256].astype(F32) + quarter_rows(decays_of(got[r, 256:272]), x) * total
        before = jnp.where(jnp.logical_or(straight, jnp.logical_not(partner)), total, beyond)
        mine_first = first_of(r == 1, x)
        first = jnp.where(mine_first, own[0:256], other[0:256].astype(F32))
        a_first = jnp.where(mine_first, decays_of(own[256:272]), decays_of(other[256:272]))
        after_x = first + quarter_rows(a_first, x) * before
        keep_ref[r] = jnp.where(mine_first, before, after_x)
        send_ref[r] = jnp.where(mine_first, after_x, before).astype(BF)


def k_slab(mine, other, own_n, got_n, own_p, got_p, keep_ref, send_ref, scratch):
    core, x = lax.axis_index("c"), lax.axis_index("xl")
    for r, (own, got) in enumerate(((own_n, got_n), (own_p, got_p))):
        scratch[x] = mine[r]
        scratch[1 - x] = other[r].astype(F32)
        before = jnp.concatenate([scratch[0], scratch[1]], axis=0)
        mine_first = first_of(r == 1, core)
        first = jnp.where(mine_first, own[0:512], got[0:512].astype(F32))
        a_first = jnp.where(mine_first, decays_of(own[512:528]), decays_of(got[512:528]))
        after_c = first + per_row(a_first, 8) * before
        keep_ref[r] = jnp.where(mine_first, before, after_c).astype(BF)
        send_ref[r] = jnp.where(mine_first, after_c, before).astype(BF)


SWAP = [(0, 1), (1, 0)]
HALF, QUARTER, TAILED = (512, 128), (256, 128), (272, 128)


def neighbour(z, x, odd, wrap):
    if not odd:
        return z ^ 1, x
    other = z + 1 if z & 1 else z - 1
    if wrap:
        return other % 8, x
    return (other, x) if 0 <= other < 8 else (z, 1 - x)


def along_z(array, step, wrap=False):
    pairs = []
    for z in range(8):
        for x in range(2):
            for c in range(2):
                z2, x2 = neighbour(z, x, (step + c) % 2, wrap)
                pairs.append((4 * z + 2 * x + c, 4 * z2 + 2 * x2 + c))
    return lax.ppermute(array, SEQ, pairs)


def core_sum(reverse, tag, keep, send):
    got = lax.ppermute(send, "c", SWAP)
    outs = (sds(TAILED, F32), sds(TAILED, BF))
    own_q, send_q = call(functools.partial(k_core, reverse), outs, "core" + tag, 0, (keep, got), [pltpu.VMEM((2,) + TAILED, F32)])
    return got, own_q, send_q


def inside(reverse, tag, lengths, skip, parts, values, bc):
    cum, cum_t, dt_t, _ = parts
    args = (lengths, skip, cum, cum_t, dt_t, values) + bc
    scratch = [pltpu.VMEM((T, T), F32), pltpu.VMEM((T, T), F32)]
    return call(functools.partial(k_inside, reverse), sds((T, 1024), F32), "inside" + tag, 2, args, scratch, us=3)


def final(reverse, tag, base, late, state, bc):
    args = (base, late) + tuple(state) + bc
    kernel = functools.partial(k_final, reverse)
    return call(kernel, sds((T, 1024), BF), "final" + tag, 0, args, [pltpu.VMEM((2, 512, 128), BF)], us=2)


def project(name, step, last, args):
    outs = (sds((T, 128), BF), sds((T, 128), F32)) if last else sds((T, 256), F32)
    return call(functools.partial(k_project, step, last), outs, name, 0, args, limit=16)


def body(hidden, values, seg_next, proj_bc, proj_dt, dt_bias, decay, skip, bc_prev, dt_prev, seg_prev, grads):
    decay_row, bias_row = decay[None, :], dt_bias[None, :]
    wide = sds((T, 128), BF)

    send = call(k_columns, sds((2, 8, 36, 128), BF), "columns", 0, (proj_bc, proj_dt)).reshape(16, 36, 128)
    got = lax.all_to_all(send, ("xl",) + FSDP, 0, 0, tiled=False)
    w0 = call(k_rows, sds((2, 288, 128), BF), "rows", 0, (got,))

    w1 = along_z(w0, 0, True)
    hid = pl.pallas_call(
        k_load,
        out_shape=sds(hidden.shape, BF),
        in_specs=[pl.BlockSpec(memory_space=pl.ANY)],
        out_specs=VM,
        name="load",
        compiler_params=pltpu.CompilerParams(vmem_limit_bytes=6 << 20),
        cost_estimate=pl.CostEstimate(flops=30_000_000, bytes_accessed=4_000_000, transcendentals=0),
    )(after(hidden, w0))
    args = (after(seg_prev, w0), dt_prev.T, decay_row, bc_prev, grads)
    local = call(k_local_prev, LOCAL_OUTS, "local_prev", 1, args, [pltpu.VMEM((2, 528, 128), F32)], us=3)
    keep_p, parts_prev = local[0], local[2:6]
    b0 = call(k_pack, sds((4, 288, 128), BF), "pack", 0, (w0, after(w1, local[1], hid)))
    b1 = along_z(b0, 1, True)
    g0 = lax.ppermute(b0, "c", SWAP)
    got_p, own_qp, send_qp = core_sum(True, "_prev", keep_p, local[1])
    b1 = after(b1, g0, send_qp)
    b2 = along_z(b1, 0, True)
    g1 = lax.ppermute(b1, "c", SWAP)
    got_qp = lax.ppermute(send_qp, "xl", SWAP)
    plane_p = call(k_chip_prev, sds(TAILED, F32), "chip_prev", 0, (own_qp, got_qp))
    acc = project("project0", (0, 1), False, (hid, b0, g0, b1, g1))
    b2 = after(b2, g1, plane_p, acc)
    b3 = along_z(b2, 1, True)
    g2 = lax.ppermute(b2, "c", SWAP)
    acc = project("project2", (2,), False, (hid, acc, b2, g2))
    base_prev = inside(True, "_prev", seg_prev, skip, parts_prev, grads, (bc_prev,))
    b3 = after(b3, acc, base_prev)
    g3 = lax.ppermute(b3, "c", SWAP)
    mine, dt_raw = project("project3", (3,), True, (hid, acc, b3, g3))

    pair = lax.ppermute(mine, "y", [(i, i ^ 1) for i in range(4)])
    args = (seg_next, dt_raw, decay_row, bias_row, mine, pair, values)
    local = call(k_local_next, LOCAL_OUTS + (wide, wide), "local_next", 1, args, [pltpu.VMEM((2, 528, 128), F32)], us=3)
    keep_n, parts_next, bc_next = local[0], local[2:6], (local[6], local[7])
    got_n, own_qn, send_qn = core_sum(False, "_next", keep_n, local[1])
    got_qn = lax.ppermute(send_qn, "xl", SWAP)
    base_next = inside(False, "_next", seg_next, skip, parts_next, values, bc_next)
    both = (sds(TAILED, F32), sds((2,) + TAILED, BF))
    plane_n, msg = call(k_chip_next, both, "chip_next", 0, (own_qn, after(got_qn, base_next), plane_p))
    m1 = along_z(msg, 0)
    m = [call(k_pairs, sds(TAILED, BF), "pairs", 0, (plane_n, plane_p, m1))]
    for step in range(1, 5):
        m.append(along_z(m[-1], step))
    both = (sds((2,) + QUARTER, F32), sds((2,) + QUARTER, BF))
    keep_q, out_q = call(k_planes, both, "planes", 0, (m1, *m[1:], own_qn, got_qn, own_qp, got_qp))
    back_q = lax.ppermute(out_q, "xl", SWAP)
    both = (sds((2,) + HALF, BF), sds((2,) + HALF, BF))
    args = (keep_q, back_q, keep_n, got_n, keep_p, got_p)
    keep_h, out_h = call(k_slab, both, "slab", 0, args, [pltpu.VMEM((2,) + QUARTER, F32)])
    state = (keep_h, lax.ppermute(out_h, "c", SWAP))
    out_next = final(False, "_next", base_next, parts_next[3], state, bc_next)
    grad_values = final(True, "_prev", base_prev, parts_prev[3], state, (bc_prev,))
    return out_next, grad_values


def solution(mesh):
    split = Mesh(mesh.devices.reshape(8, 2, 2, 2, 4), ("z", "xl", "c", "xh", "y"))
    all_axes = SEQ + FSDP
    in_specs = (
        P(SEQ, None),
        P(SEQ, FSDP),
        P(),
        P(all_axes, None),
        P(all_axes, None),
        P(),
        P(),
        P(),
        P(SEQ, None),
        P(SEQ, FSDP),
        P(),
        P(SEQ, FSDP),
    )
    out_specs = (P(SEQ, FSDP), P(SEQ, FSDP))
    return jax.shard_map(body, mesh=split, in_specs=in_specs, out_specs=out_specs, check_vma=False)
```
